256 devices in a mesh: doc: 8 (over y_lo, x), ctx: 32 (over z, y_hi, core).
Axes of the slice: x: 4, y: 4 (y_hi: 2, y_lo: 2; y = y_hi * 2 + y_lo), z: 8, core: 2. Of those that a mesh axis runs over, the one named last changes fastest.
Arguments:
- queries: bfloat16 [8, 8192, 32, 128], P('doc', 'ctx'), may hold values from -6 to 6
- stored_key_state: bfloat16 [8, 8192, 4, 128], P('doc', 'ctx'), may hold values from -6 to 6
- stored_value_state: bfloat16 [8, 8192, 4, 128], P('doc', 'ctx'), may hold values from -0.5390625 to 0.5390625
- out_grad: bfloat16 [8, 8192, 32, 128], P('doc', 'ctx'), may hold values from -6 to 6
- logsumexp: float32 [8, 32, 8192], P('doc', None, 'ctx'), may hold values from 3 to 5
- row_dots: float32 [8, 32, 8192], P('doc', None, 'ctx'), may hold values from -6 to 6
Outputs:
- query_grad: float32 [8, 8192, 32, 128], P('doc', 'ctx')
- key_grad: float32 [8, 8192, 4, 128], P('doc', 'ctx')
- value_grad: float32 [8, 8192, 4, 128], P('doc', 'ctx')
The draws below stay inside these ranges and needn't reach their ends.
All inputs are finite; a program needn't handle non-finite values.
Results may differ from the reference program's by a relative error of at most 0.0053.
Values may be sent and summed in bfloat16 or wider, within the bound.
No kernel may reach another device: no remote copies, remote signals or barrier semaphores. Data moves between devices by JAX's collectives and lax.ppermute only.
A program may use at most 64 MiB of HBM per device.

```python
import jax
import jax.numpy as jnp
from jax import lax

HQ = 32
KEY_VALUE_HEADS = 4
HEAD_SIZE = 128
BLOCK_TOKENS = 256
DOCUMENT_COUNT = 8
DOCUMENT_TOKENS = 8192


def shard_levels(stream_key, shape, cuts, least, top_value):
    def one(position, blocks):
        draws = jax.random.uniform(jax.random.fold_in(jax.random.fold_in(stream_key, 6), position), (blocks,), jnp.float32, least / len(cuts), top_value / len(cuts))
        return jnp.repeat(jnp.exp(draws), shape[position] // blocks).reshape((-1,) + (1,) * (len(shape) - position - 1))

    factor_of = one(*cuts[0])
    for cut in cuts[1:]:
        factor_of = factor_of * one(*cut)
    return factor_of


def scatter_about(rng, extent, deviation, most, shards=(), held_as=jnp.bfloat16):
    loudness = shard_levels(rng, extent, shards, -0.22, 0.18) if shards else 1.0
    values = jax.random.normal(rng, extent, jnp.float32) * deviation * loudness
    return jnp.minimum(jnp.maximum(values, -most), most).astype(held_as)


def setup_inputs(seed: int = 0) -> dict:
    key_list = jax.random.split(jax.random.key(seed), 7)
    queries = scatter_about(key_list[0], (DOCUMENT_COUNT, DOCUMENT_TOKENS, HQ, HEAD_SIZE), 1.0, 6.0, ((0, 8), (1, 32)))
    stored_key_state = scatter_about(key_list[1], (DOCUMENT_COUNT, DOCUMENT_TOKENS, KEY_VALUE_HEADS, HEAD_SIZE), 1.0, 6.0, ((0, 8), (1, 32)))
    stored_value_state = scatter_about(key_list[2], (DOCUMENT_COUNT, DOCUMENT_TOKENS, KEY_VALUE_HEADS, HEAD_SIZE), 0.09, 0.5390625, ((0, 8), (1, 32)))
    out_grad = scatter_about(key_list[3], (DOCUMENT_COUNT, DOCUMENT_TOKENS, HQ, HEAD_SIZE), 1.0, 6.0, ((0, 8), (1, 32)))
    logsumexp = jnp.clip(3.0 + 2.0 * jax.random.uniform(key_list[4], (DOCUMENT_COUNT, HQ, DOCUMENT_TOKENS), jnp.float32) ** shard_levels(key_list[4], (DOCUMENT_COUNT, HQ, DOCUMENT_TOKENS), ((0, 8), (2, 32)), -0.2, 0.2), 3.0, 5.0)
    row_dots = scatter_about(key_list[5], (DOCUMENT_COUNT, HQ, DOCUMENT_TOKENS), 1.0, 6.0, ((0, 8), (2, 32)), jnp.float32)
    return {"queries": queries, "stored_key_state": stored_key_state, "stored_value_state": stored_value_state, "out_grad": out_grad, "logsumexp": logsumexp, "row_dots": row_dots}


def score_mask(block_index, length):
    query_pos = lax.broadcasted_iota(jnp.int32, (length, 5 * length), 0)
    key_slot = lax.broadcasted_iota(jnp.int32, (length, 5 * length), 1)
    source = key_slot // length
    within = key_slot % length
    causal = (source == 2) & (within <= query_pos)
    older = ((source == 0) | (source == 3)) & (block_index >= 2)
    recent = ((source == 1) | (source == 4)) & (block_index >= 1)
    return causal | older | recent


def block_backward(query_rows, grad_rows, lse_rows, dot_rows, keys_all, values_all, allowed):
    length, heads, width = query_rows.shape
    groups = keys_all.shape[1]
    per_group = heads // groups
    scaling = width ** -0.5
    query_split = query_rows.reshape(length, groups, per_group, width).astype(jnp.float32)
    grad_split = grad_rows.reshape(length, groups, per_group, width).astype(jnp.float32)
    lse_split = lse_rows.reshape(groups, per_group, length)
    dot_split = dot_rows.reshape(groups, per_group, length)
    keys_float = keys_all.astype(jnp.float32)
    values_float = values_all.astype(jnp.float32)

    def one_group(group_index):
        query_head = lax.dynamic_index_in_dim(query_split, group_index, 1, keepdims=False)
        grad_head = lax.dynamic_index_in_dim(grad_split, group_index, 1, keepdims=False)
        key_head = lax.dynamic_index_in_dim(keys_float, group_index, 1, keepdims=False)
        value_head = lax.dynamic_index_in_dim(values_float, group_index, 1, keepdims=False)
        lse_head = lax.dynamic_index_in_dim(lse_split, group_index, 0, keepdims=False)
        dot_head = lax.dynamic_index_in_dim(dot_split, group_index, 0, keepdims=False)
        scores = jnp.einsum("igd,md->gim", query_head, key_head) * scaling
        probs = jnp.where(allowed[None], jnp.exp(scores - lse_head[:, :, None]), jnp.float32(0.0))
        probs_half = lax.optimization_barrier(probs.astype(jnp.bfloat16)).astype(jnp.float32)
        value_part = jnp.einsum("gim,igd->md", probs_half, grad_head)
        prob_grad = jnp.einsum("igd,md->gim", grad_head, value_head)
        score_grad = (probs * (prob_grad - dot_head[:, :, None])).astype(jnp.bfloat16)
        score_grad = lax.optimization_barrier(score_grad).astype(jnp.float32)
        query_part = jnp.einsum("gim,md->igd", score_grad, key_head) * scaling
        key_part = jnp.einsum("gim,igd->md", score_grad, query_head) * scaling
        return query_part, key_part, value_part

    query_part, key_part, value_part = lax.map(one_group, jnp.arange(groups, dtype=jnp.int32))
    query_out = jnp.transpose(query_part, (1, 0, 2, 3)).reshape(length, heads, width)
    return query_out, jnp.transpose(key_part, (1, 0, 2)), jnp.transpose(value_part, (1, 0, 2))


def later_blocks(blocks, steps):
    return jnp.concatenate([blocks[:, steps:], jnp.zeros_like(blocks[:, :steps])], axis=1)


def assemble(collected_rows, context_block_count):
    split_parts = collected_rows.reshape(DOCUMENT_COUNT, context_block_count, 5, BLOCK_TOKENS, KEY_VALUE_HEADS, HEAD_SIZE)
    own_sum = split_parts[:, :, 2] + later_blocks(split_parts[:, :, 1], 1) + later_blocks(split_parts[:, :, 0], 2)
    partner_sum = later_blocks(split_parts[:, :, 4], 1) + later_blocks(split_parts[:, :, 3], 2)
    reduced_sum = own_sum + jnp.roll(partner_sum, 1, axis=0)
    return reduced_sum.reshape(DOCUMENT_COUNT, DOCUMENT_TOKENS, KEY_VALUE_HEADS, HEAD_SIZE)


def reference(queries, stored_key_state, stored_value_state, out_grad, logsumexp, row_dots):
    context_block_count = DOCUMENT_TOKENS // BLOCK_TOKENS
    stacked_rows = jnp.stack([stored_key_state, stored_value_state], axis=1)
    padded_rows = jnp.concatenate([jnp.zeros((DOCUMENT_COUNT, 2, 2 * BLOCK_TOKENS, KEY_VALUE_HEADS, HEAD_SIZE), jnp.bfloat16), stacked_rows], axis=2)

    def one_item(item_index):
        document = item_index // context_block_count
        block_index = item_index % context_block_count
        partner = (document + 1) % DOCUMENT_COUNT
        offset = (block_index * BLOCK_TOKENS).astype(jnp.int32)
        own_rows = lax.dynamic_index_in_dim(padded_rows, document, 0, keepdims=False)
        theirs = lax.dynamic_index_in_dim(padded_rows, partner, 0, keepdims=False)
        own_span = lax.dynamic_slice_in_dim(own_rows, offset, 3 * BLOCK_TOKENS, 1)
        part_span = lax.dynamic_slice_in_dim(theirs, offset, 2 * BLOCK_TOKENS, 1)
        joined = jnp.concatenate([own_span, part_span], axis=1)
        zero = jnp.int32(0)
        query_rows = lax.dynamic_slice(queries, (document, offset, zero, zero), (1, BLOCK_TOKENS, HQ, HEAD_SIZE))[0]
        grad_rows = lax.dynamic_slice(out_grad, (document, offset, zero, zero), (1, BLOCK_TOKENS, HQ, HEAD_SIZE))[0]
        lse_rows = lax.dynamic_slice(logsumexp, (document, zero, offset), (1, HQ, BLOCK_TOKENS))[0]
        dot_rows = lax.dynamic_slice(row_dots, (document, zero, offset), (1, HQ, BLOCK_TOKENS))[0]
        allowed = score_mask(block_index, BLOCK_TOKENS)
        return block_backward(query_rows, grad_rows, lse_rows, dot_rows, joined[0], joined[1], allowed)

    query_all, key_all, value_all = lax.map(one_item, jnp.arange(DOCUMENT_COUNT * context_block_count, dtype=jnp.int32))
    query_grad = query_all.reshape(DOCUMENT_COUNT, DOCUMENT_TOKENS, HQ, HEAD_SIZE)
    return query_grad, assemble(key_all, context_block_count), assemble(value_all, context_block_count)
```

```python
import functools
import math

import jax
import jax.numpy as jnp
from jax import lax
from jax.experimental import pallas as pl
from jax.experimental.pallas import tpu as pltpu
from jax.sharding import PartitionSpec as P

LOG2E = math.log2(math.e)
F32, BF16 = jnp.float32, jnp.bfloat16
NT = (((1,), (1,)), ((), ()))
NN = (((1,), (0,)), ((), ()))
TN = (((0,), (0,)), ((), ()))


def mm(a, b, dims):
    return lax.dot_general(a, b, dims, preferred_element_type=F32)


def columns(width, q, g, lse_ref, dot_ref, sl, k, v, mask):
    qc, gc = q[sl, :], g[sl, :]
    s = mm(k, qc, NT)
    p = jnp.exp2(s * (LOG2E * width**-0.5) - lse_ref[0, :, sl])
    if mask is not None:
        p = jnp.where(mask, p, 0.0)
    dv = mm(p.astype(BF16), gc, NN)
    dp = mm(v, gc, NT)
    ds = (p * (dp - dot_ref[0, :, sl])).astype(BF16)
    dk = mm(ds, qc, NN)
    dq = mm(ds, k, TN)
    return dq, dk, dv


def pair_kernel(cw, n_near, first, q_ref, g_ref, lse_ref, dot_ref, far_ref, *rest):
    near_refs, rest = rest[:n_near], rest[n_near:]
    prev_ref = None
    if not first:
        prev_ref, *rest = rest
    dq_ref, near_out, far_out = rest
    tokens, heads, width = q_ref.shape
    n = tokens * heads
    q, g = q_ref.reshape(n, width), g_ref.reshape(n, width)
    near_k, near_v = near_refs[0][0, 0], near_refs[0][1, 0]
    for other in near_refs[1:]:
        near_k, near_v = near_k + other[0, 0], near_v + other[1, 0]
    k = jnp.concatenate([far_ref[0, 0], near_k], axis=0)
    v = jnp.concatenate([far_ref[1, 0], near_v], axis=0)
    dk = dv = None
    for c in range(n // cw):
        sl = pl.ds(c * cw, cw)
        dqc, dkc, dvc = columns(width, q, g, lse_ref, dot_ref, sl, k, v, None)
        if prev_ref is not None:
            dqc = dqc + prev_ref.reshape(n, width)[sl, :]
        dq_ref.reshape(n, width)[sl, :] = dqc
        dk = dkc if dk is None else dk + dkc
        dv = dvc if dv is None else dv + dvc
    dk = dk * width**-0.5
    far_out[0, 0] = dk[:tokens]
    far_out[1, 0] = dv[:tokens]
    near_out[0, 0] = dk[tokens:].astype(BF16)
    near_out[1, 0] = dv[tokens:].astype(BF16)


def own_kernel(cw, q_ref, g_ref, lse_ref, dot_ref, kv_ref, prev_ref, dq_ref, own_out):
    tokens, heads, width = q_ref.shape
    n = tokens * heads
    q, g = q_ref.reshape(n, width), g_ref.reshape(n, width)
    own_out[...] = jnp.zeros_like(own_out)
    for c in range(n // cw):
        sl = pl.ds(c * cw, cw)
        seen = (c + 1) * cw // heads
        k, v = kv_ref[0, 0, :seen, :], kv_ref[1, 0, :seen, :]
        key = lax.broadcasted_iota(jnp.int32, (seen, cw), 0)
        column = lax.broadcasted_iota(jnp.int32, (seen, cw), 1) + c * cw
        dqc, dkc, dvc = columns(width, q, g, lse_ref, dot_ref, sl, k, v, key * heads <= column)
        dqc = dqc + prev_ref.reshape(n, width)[sl, :]
        dq_ref.reshape(n, width)[sl, :] = dqc * width**-0.5
        own_out[0, 0, :seen, :] += dkc * width**-0.5
        own_out[1, 0, :seen, :] += dvc


def specs(tokens, heads, groups, width):
    per = heads // groups
    row = pl.BlockSpec((tokens, per, width), lambda j: (0, j, 0))
    vec = pl.BlockSpec((1, 1, tokens * per), lambda j: (j, 0, 0))
    blk = pl.BlockSpec((2, 1, tokens, width), lambda j: (0, j, 0, 0))
    return row, vec, blk


def pair_call(name, q, g, lse, dots, far, nears, prev):
    tokens, heads, width = q.shape
    groups = far.shape[1]
    row, vec, blk = specs(tokens, heads, groups, width)
    pairs = 2 * tokens * heads * tokens
    args = [q, g, lse, dots, far, *nears] + ([] if prev is None else [prev])
    return pl.pallas_call(
        functools.partial(pair_kernel, 512, len(nears), prev is None),
        grid=(groups,),
        in_specs=[row, row, vec, vec, blk] + [blk] * len(nears) + ([] if prev is None else [row]),
        out_specs=[row, blk, blk],
        out_shape=[
            jax.ShapeDtypeStruct(q.shape, F32),
            jax.ShapeDtypeStruct(far.shape, BF16),
            jax.ShapeDtypeStruct(far.shape, F32),
        ],
        compiler_params=pltpu.CompilerParams(dimension_semantics=("arbitrary",)),
        cost_estimate=pl.CostEstimate(
            flops=10 * pairs * width, transcendentals=pairs, bytes_accessed=16 << 20
        ),
        name=name,
    )(*args)


def own_call(q, g, lse, dots, kv, prev):
    tokens, heads, width = q.shape
    groups = kv.shape[1]
    row, vec, blk = specs(tokens, heads, groups, width)
    pairs = tokens * heads * tokens
    return pl.pallas_call(
        functools.partial(own_kernel, 512),
        grid=(groups,),
        in_specs=[row, row, vec, vec, blk, row],
        out_specs=[row, blk],
        out_shape=[jax.ShapeDtypeStruct(q.shape, F32), jax.ShapeDtypeStruct(kv.shape, F32)],
        compiler_params=pltpu.CompilerParams(dimension_semantics=("arbitrary",)),
        cost_estimate=pl.CostEstimate(
            flops=10 * pairs * width, transcendentals=pairs, bytes_accessed=16 << 20
        ),
        name="own",
    )(q, g, lse, dots, kv, prev)


def send(x, by_doc, to):
    docs, ctxs = lax.axis_size("doc"), lax.axis_size("ctx")
    pairs = []
    for d in range(docs):
        for c in range(ctxs):
            t = to(c)
            if t is not None and 0 <= t < ctxs:
                pairs.append((d * ctxs + c, (d + by_doc) % docs * ctxs + t))
    return lax.ppermute(x, ("doc", "ctx"), pairs)


def ahead(c):
    return c + 2


def back(c):
    return c - 2


def swap(c):
    return c ^ 1


def even_to_odd(c):
    return c + 1 if c % 2 == 0 else None


def odd_to_even(c):
    return c - 1 if c % 2 == 1 else None


def by_group(x, groups):
    heads, tokens = x.shape
    return x.reshape(groups, heads // groups, tokens).transpose(0, 2, 1).reshape(groups, 1, -1)


def per_device(queries, stored_key_state, stored_value_state, out_grad, logsumexp, row_dots):
    groups = stored_key_state.shape[2]
    q, g = queries[0], out_grad[0]
    odd = lax.axis_index("ctx") % 2 == 1
    kv = jnp.stack([stored_key_state[0], stored_value_state[0]]).transpose(0, 2, 1, 3)

    part_far = send(kv, -1, ahead)
    part_near_odd = send(kv, -1, even_to_odd)
    part_near_even = send(part_far, 0, odd_to_even)
    kv_later, _ = lax.optimization_barrier((kv, part_far))
    own_far = send(kv_later, 0, ahead)
    own_near = send(jnp.where(odd, own_far, kv), 0, swap)

    lse = by_group(logsumexp[0] * LOG2E, groups)
    dots = by_group(row_dots[0], groups)

    dq, part_near_grad, part_far_grad = pair_call(
        "partner", q, g, lse, dots, part_far, [part_near_odd, part_near_even], None
    )
    near_home = send(part_near_grad, 1, odd_to_even)
    near_mate = send(part_near_grad, 0, even_to_odd)
    part_home = send((part_far_grad + near_mate.astype(F32)).astype(BF16), 1, back)

    dq, own_near_grad, own_far_grad = pair_call(
        "earlier", q, g, lse, dots, own_far, [own_near], dq
    )
    swapped = send(own_near_grad, 0, swap).astype(F32)
    own_home = send((own_far_grad + jnp.where(odd, swapped, 0.0)).astype(BF16), 0, back)

    dq, own_grad = own_call(q, g, lse, dots, kv, dq)
    total = own_grad + jnp.where(odd, 0.0, swapped) + near_home.astype(F32)
    total = total + part_home.astype(F32) + own_home.astype(F32)
    total = total.transpose(0, 2, 1, 3)
    return dq[None], total[0][None], total[1][None]


def solution(mesh):
    rows, vecs = P("doc", "ctx", None, None), P("doc", None, "ctx")
    return jax.shard_map(
        per_device,
        mesh=mesh,
        in_specs=(rows, rows, rows, rows, vecs, vecs),
        out_specs=(rows, rows, rows),
        check_vma=False,
    )
```

```python
import functools
import math

import jax
import jax.numpy as jnp
from jax import lax
from jax.experimental import pallas as pl
from jax.experimental.pallas import tpu as pltpu
from jax.sharding import PartitionSpec as P


LOG2E = math.log2(math.e)
F32, BF16 = jnp.float32, jnp.bfloat16
NT = (((1,), (1,)), ((), ()))
NN = (((1,), (0,)), ((), ()))
TN = (((0,), (0,)), ((), ()))


def mm(a, b, dims):
    return lax.dot_general(a, b, dims, preferred_element_type=F32)


def columns(width, q, g, lse_ref, dot_ref, sl, k, v, mask):
    qc, gc = q[sl, :], g[sl, :]
    s = mm(k, qc, NT)
    p = jnp.exp2(s * (LOG2E * width**-0.5) - lse_ref[0, :, sl])
    if mask is not None:
        p = jnp.where(mask, p, 0.0)
    dv = mm(p.astype(BF16), gc, NN)
    dp = mm(v, gc, NT)
    ds = (p * (dp - dot_ref[0, :, sl])).astype(BF16)
    dk = mm(ds, qc, NN)
    dq = mm(ds, k, TN)
    return dq, dk, dv


def earlier_kernel(cw, merge, last, q_ref, g_ref, lse_ref, dot_ref, prev_ref, *rest):
    n_in = sum(merge)
    in_refs, dq_ref, outs = rest[:n_in], rest[n_in], rest[n_in + 1 :]
    tokens, heads, width = q_ref.shape
    n = tokens * heads
    q, g = q_ref.reshape(n, width), g_ref.reshape(n, width)
    blocks = []
    for count in merge:
        k, v = in_refs[0][0, 0], in_refs[0][1, 0]
        for other in in_refs[1:count]:
            k, v = k + other[0, 0], v + other[1, 0]
        blocks.append((k, v))
        in_refs = in_refs[count:]
    k = jnp.concatenate([k for k, _ in blocks], axis=0)
    v = jnp.concatenate([v for _, v in blocks], axis=0)
    dk = dv = None
    for c in range(n // cw):
        sl = pl.ds(c * cw, cw)
        dqc, dkc, dvc = columns(width, q, g, lse_ref, dot_ref, sl, k, v, None)
        dqc = dqc + prev_ref.reshape(n, width)[sl, :]
        dq_ref.reshape(n, width)[sl, :] = dqc * width**-0.5 if last else dqc
        dk = dkc if dk is None else dk + dkc
        dv = dvc if dv is None else dv + dvc
    dk = dk * width**-0.5
    for i, out in enumerate(outs):
        out[0, 0] = dk[i * tokens : (i + 1) * tokens].astype(BF16)
        out[1, 0] = dv[i * tokens : (i + 1) * tokens].astype(BF16)


def own_kernel(cw, step, q_ref, g_ref, lse_ref, dot_ref, kv_ref, dq_ref, own_out):
    tokens, heads, width = q_ref.shape
    n = tokens * heads
    q, g = q_ref.reshape(n, width), g_ref.reshape(n, width)
    parts = []
    for c in range(n // cw):
        sl = pl.ds(c * cw, cw)
        seen = pl.cdiv((c + 1) * cw // heads, step) * step
        k, v = kv_ref[0, 0, :seen, :], kv_ref[1, 0, :seen, :]
        key = lax.broadcasted_iota(jnp.int32, (seen, cw), 0)
        column = lax.broadcasted_iota(jnp.int32, (seen, cw), 1) + c * cw
        dqc, dkc, dvc = columns(width, q, g, lse_ref, dot_ref, sl, k, v, key * heads <= column)
        dq_ref.reshape(n, width)[sl, :] = dqc
        parts.append((dkc * width**-0.5, dvc))
    done = 0
    for seen in sorted({dk.shape[0] for dk, _ in parts}):
        rows = [(dk[done:seen], dv[done:seen]) for dk, dv in parts if dk.shape[0] >= seen]
        own_out[0, 0, done:seen, :] = sum(dk for dk, _ in rows)
        own_out[1, 0, done:seen, :] = sum(dv for _, dv in rows)
        done = seen


def specs(tokens, heads, groups, width):
    per = heads // groups
    row = pl.BlockSpec((tokens, per, width), lambda j: (0, j, 0))
    vec = pl.BlockSpec((1, 1, tokens * per), lambda j: (j, 0, 0))
    blk = pl.BlockSpec((2, 1, tokens, width), lambda j: (0, j, 0, 0))
    return row, vec, blk


def earlier_call(q, g, lse, dots, prev, blocks, last):
    tokens, heads, width = q.shape
    groups = blocks[0][0].shape[1]
    row, vec, blk = specs(tokens, heads, groups, width)
    pairs = len(blocks) * tokens * heads * tokens
    parts = [part for block in blocks for part in block]
    merge = tuple(len(block) for block in blocks)
    return pl.pallas_call(
        functools.partial(earlier_kernel, 512 if len(blocks) > 1 else 1024, merge, last),
        grid=(groups,),
        in_specs=[row, row, vec, vec, row] + [blk] * len(parts),
        out_specs=[row] + [blk] * len(blocks),
        out_shape=[jax.ShapeDtypeStruct(q.shape, F32)]
        + [jax.ShapeDtypeStruct(parts[0].shape, BF16)] * len(blocks),
        compiler_params=pltpu.CompilerParams(dimension_semantics=("arbitrary",)),
        cost_estimate=pl.CostEstimate(
            flops=10 * pairs * width, transcendentals=pairs, bytes_accessed=16 << 20
        ),
    )(q, g, lse, dots, prev, *parts)


def own_call(q, g, lse, dots, kv):
    tokens, heads, width = q.shape
    groups = kv.shape[1]
    row, vec, blk = specs(tokens, heads, groups, width)
    pairs = tokens * heads * tokens
    return pl.pallas_call(
        functools.partial(own_kernel, 1024, 128),
        grid=(groups,),
        in_specs=[row, row, vec, vec, blk],
        out_specs=[row, blk],
        out_shape=[jax.ShapeDtypeStruct(q.shape, F32), jax.ShapeDtypeStruct(kv.shape, F32)],
        compiler_params=pltpu.CompilerParams(dimension_semantics=("arbitrary",)),
        cost_estimate=pl.CostEstimate(
            flops=10 * pairs * width, transcendentals=pairs, bytes_accessed=16 << 20
        ),
        name="own",
    )(q, g, lse, dots, kv)


def send(x, by_doc, to):
    docs, ctxs = lax.axis_size("doc"), lax.axis_size("ctx")
    pairs = []
    for d in range(docs):
        for c in range(ctxs):
            t = to(c)
            if t is not None and 0 <= t < ctxs:
                pairs.append((d * ctxs + c, (d + by_doc) % docs * ctxs + t))
    return lax.ppermute(x, ("doc", "ctx"), pairs)


def ahead(c):
    return c + 2


def back_one(c):
    return c - 1


def back_two(c):
    return c - 2


def swap(c):
    return c ^ 1


def even_to_odd(c):
    return c + 1 if c % 2 == 0 else None


def odd_to_even(c):
    return c - 1 if c % 2 == 1 else None


def by_group(x, groups):
    heads, tokens = x.shape
    return x.reshape(groups, heads // groups, tokens).transpose(0, 2, 1).reshape(groups, 1, -1)


def step(queries, stored_key_state, stored_value_state, out_grad, logsumexp, row_dots):
    groups = stored_key_state.shape[2]
    q, g = queries[0], out_grad[0]
    odd = lax.axis_index("ctx") % 2 == 1
    kv = jnp.stack([stored_key_state[0], stored_value_state[0]]).transpose(0, 2, 1, 3)

    part_far = send(kv, -1, ahead)
    part_near_odd = send(kv, -1, even_to_odd)
    own_far = send(kv, 0, ahead)
    part_near_even = send(part_far, 0, odd_to_even)

    lse = by_group(logsumexp[0] * LOG2E, groups)
    dots = by_group(row_dots[0], groups)
    dq, own_grad = own_call(q, g, lse, dots, kv)
    dq, far_grad, near_grad = earlier_call(
        q, g, lse, dots, dq, [[part_far], [part_near_odd, part_near_even]], False
    )
    own_far, dq = lax.optimization_barrier((own_far, dq))
    part_far_home = send(far_grad, 1, back_two)
    part_near_home = send(near_grad, 1, back_one)
    own_near = send(jnp.where(odd, own_far, kv), 0, swap)
    dq, far_grad = earlier_call(q, g, lse, dots, dq, [[own_far]], False)
    own_far_home = send(far_grad, 0, back_two)
    dq, near_grad = earlier_call(q, g, lse, dots, dq, [[own_near]], True)
    own_near_home = send(near_grad, 0, back_one)

    total = own_grad + part_far_home.astype(F32) + part_near_home.astype(F32)
    total = total + own_far_home.astype(F32) + own_near_home.astype(F32)
    total = total.transpose(0, 2, 1, 3)
    return dq[None], total[0][None], total[1][None]


def solution(mesh):
    rows, vecs = P("doc", "ctx", None, None), P("doc", None, "ctx")
    return jax.shard_map(
        step,
        mesh=mesh,
        in_specs=(rows, rows, rows, rows, vecs, vecs),
        out_specs=(rows, rows, rows),
        check_vma=False,
    )
```

```python
import functools
import math

import jax
import jax.numpy as jnp
from jax import lax
from jax.experimental import pallas as pl
from jax.experimental.pallas import tpu as pltpu
from jax.sharding import PartitionSpec as P


LOG2E = math.log2(math.e)
F32, BF16 = jnp.float32, jnp.bfloat16
NT = (((1,), (1,)), ((), ()))
NN = (((1,), (0,)), ((), ()))
TN = (((0,), (0,)), ((), ()))


def mm(a, b, dims):
    return lax.dot_general(a, b, dims, preferred_element_type=F32)


def columns(width, q, g, lse, dot, sl, k, v, mask):
    qc, gc = q[sl, :], g[sl, :]
    s = mm(k, qc, NT)
    p = jnp.exp2(s * (LOG2E * width**-0.5) - lse[:, sl])
    if mask is not None:
        p = jnp.where(mask, p, 0.0)
    dv = mm(p.astype(BF16), gc, NN)
    dp = mm(v, gc, NT)
    ds = (p * (dp - dot[:, sl])).astype(BF16)
    dk = mm(ds, qc, NN)
    dq = mm(ds, k, TN)
    return dq, dk, dv


def own_kernel(cw, step, q_hbm, g_hbm, lse_ref, dot_ref, kv_ref, q_ref, g_ref, dq_ref, out_ref, sems):
    groups, tokens, heads, width = q_ref.shape
    n = tokens * heads

    def copies(j):
        rows = pl.ds(pl.multiple_of(j * heads, heads), heads)
        return [
            pltpu.make_async_copy(src.at[:, rows, :], dst.at[j], sems.at[i, j])
            for i, (src, dst) in enumerate(((q_hbm, q_ref), (g_hbm, g_ref)))
        ]

    for j in range(groups):
        for copy in copies(j):
            copy.start()

    def group(j, carry):
        for copy in copies(j):
            copy.wait()
        q, g = q_ref.at[j].reshape(n, width), g_ref.at[j].reshape(n, width)
        dq_rows = dq_ref.at[j].reshape(n, width)
        parts = []
        for c in range(n // cw):
            sl = pl.ds(c * cw, cw)
            seen = pl.cdiv((c + 1) * cw // heads, step) * step
            k, v = kv_ref[0, j, :seen, :], kv_ref[1, j, :seen, :]
            key = lax.broadcasted_iota(jnp.int32, (seen, cw), 0)
            column = lax.broadcasted_iota(jnp.int32, (seen, cw), 1) + c * cw
            mask = key * heads <= column
            dqc, dkc, dvc = columns(width, q, g, lse_ref.at[j], dot_ref.at[j], sl, k, v, mask)
            dq_rows[sl, :] = dqc
            parts.append((dkc * width**-0.5, dvc))
        done = 0
        for seen in sorted({dk.shape[0] for dk, _ in parts}):
            rows = [(dk[done:seen], dv[done:seen]) for dk, dv in parts if dk.shape[0] >= seen]
            out_ref[0, j, done:seen, :] = sum(dk for dk, _ in rows)
            out_ref[1, j, done:seen, :] = sum(dv for _, dv in rows)
            done = seen
        return carry

    lax.fori_loop(0, groups, group, 0)


def earlier_kernel(cw, merge, last, q_ref, g_ref, lse_ref, dot_ref, prev_ref, *rest):
    n_in = sum(merge)
    in_refs, dq_out, rest = rest[:n_in], rest[n_in], rest[n_in + 1 :]
    outs, scratch = rest[: len(merge)], rest[len(merge) :]
    groups, tokens, heads, width = q_ref.shape
    n = tokens * heads

    def copy_out(j):
        rows = pl.ds(pl.multiple_of(j * heads, heads), heads)
        return pltpu.make_async_copy(scratch[0].at[j], dq_out.at[:, rows, :], scratch[1].at[j])

    def group(j, carry):
        q, g = q_ref.at[j].reshape(n, width), g_ref.at[j].reshape(n, width)
        prev = prev_ref.at[j].reshape(n, width)
        dq_rows = (scratch[0] if last else dq_out).at[j].reshape(n, width)
        blocks, refs = [], in_refs
        for count in merge:
            k, v = refs[0][0, j], refs[0][1, j]
            for other in refs[1:count]:
                k, v = k + other[0, j], v + other[1, j]
            blocks.append((k, v))
            refs = refs[count:]
        k = jnp.concatenate([k for k, _ in blocks], axis=0)
        v = jnp.concatenate([v for _, v in blocks], axis=0)
        dk = dv = None
        for c in range(n // cw):
            sl = pl.ds(c * cw, cw)
            dqc, dkc, dvc = columns(width, q, g, lse_ref.at[j], dot_ref.at[j], sl, k, v, None)
            dqc = dqc + prev[sl, :]
            dq_rows[sl, :] = dqc * width**-0.5 if last else dqc
            dk = dkc if dk is None else dk + dkc
            dv = dvc if dv is None else dv + dvc
        if last:
            copy_out(j).start()
        dk = dk * width**-0.5
        for i, out in enumerate(outs):
            out[0, j] = dk[i * tokens : (i + 1) * tokens].astype(BF16)
            out[1, j] = dv[i * tokens : (i + 1) * tokens].astype(BF16)
        return carry

    lax.fori_loop(0, groups, group, 0)
    if last:
        for j in range(groups):
            copy_out(j).wait()


VMEM = pl.BlockSpec(memory_space=pltpu.VMEM)
HBM = pl.BlockSpec(memory_space=pltpu.HBM)


def in_hbm(x):
    return pltpu.with_memory_space_constraint(x, pltpu.HBM)


def in_vmem(x):
    return pltpu.with_memory_space_constraint(x, pltpu.VMEM)


def work(blocks, rows, tokens, width):
    pairs = blocks * rows * tokens
    return pl.CostEstimate(flops=10 * pairs * width, transcendentals=pairs, bytes_accessed=16 << 20)


def own_call(q, g, lse, dots, kv):
    tokens, heads, width = q.shape
    groups = kv.shape[1]
    shape = (groups, tokens, heads // groups, width)
    return pl.pallas_call(
        functools.partial(own_kernel, 1024, 128),
        in_specs=[HBM, HBM, VMEM, VMEM, VMEM],
        out_specs=[VMEM, VMEM, VMEM, VMEM],
        out_shape=[
            pltpu.VMEM(shape, BF16),
            pltpu.VMEM(shape, BF16),
            pltpu.VMEM(shape, F32),
            jax.ShapeDtypeStruct(kv.shape, F32),
        ],
        scratch_shapes=[pltpu.SemaphoreType.DMA((2, groups))],
        compiler_params=pltpu.CompilerParams(vmem_limit_bytes=LIMIT),
        cost_estimate=work(1, heads * tokens, tokens, width),
        name="own",
    )(in_hbm(q), in_hbm(g), lse, dots, kv)


def earlier_call(q, g, lse, dots, prev, blocks, last):
    groups, tokens, per, width = q.shape
    parts = [part for block in blocks for part in block]
    merge = tuple(len(block) for block in blocks)
    if last:
        dq_shape = jax.ShapeDtypeStruct((tokens, groups * per, width), F32)
        scratch = [pltpu.VMEM(q.shape, F32), pltpu.SemaphoreType.DMA((groups,))]
    else:
        dq_shape, scratch = pltpu.VMEM(q.shape, F32), []
    return pl.pallas_call(
        functools.partial(earlier_kernel, 512 if len(blocks) > 1 else 1024, merge, last),
        in_specs=[VMEM] * (5 + len(parts)),
        out_specs=[HBM if last else VMEM] + [VMEM] * len(blocks),
        out_shape=[dq_shape] + [jax.ShapeDtypeStruct(parts[0].shape, BF16)] * len(blocks),
        scratch_shapes=scratch,
        input_output_aliases={} if last else {4: 0},
        compiler_params=pltpu.CompilerParams(vmem_limit_bytes=LIMIT),
        cost_estimate=work(len(blocks), groups * per * tokens, tokens, width),
    )(in_vmem(q), in_vmem(g), lse, dots, in_vmem(prev), *parts)


LIMIT = 24 << 20


def send(x, by_doc, to):
    docs, ctxs = lax.axis_size("doc"), lax.axis_size("ctx")
    pairs = []
    for d in range(docs):
        for c in range(ctxs):
            t = to(c)
            if t is not None and 0 <= t < ctxs:
                pairs.append((d * ctxs + c, (d + by_doc) % docs * ctxs + t))
    return lax.ppermute(x, ("doc", "ctx"), pairs)


def ahead(c):
    return c + 2


def back_one(c):
    return c - 1


def back_two(c):
    return c - 2


def swap(c):
    return c ^ 1


def even_to_odd(c):
    return c + 1 if c % 2 == 0 else None


def odd_to_even(c):
    return c - 1 if c % 2 == 1 else None


def by_group(x, groups):
    heads, tokens = x.shape
    return x.reshape(groups, heads // groups, tokens).transpose(0, 2, 1).reshape(groups, 1, -1)


def step(queries, stored_key_state, stored_value_state, out_grad, logsumexp, row_dots):
    groups = stored_key_state.shape[2]
    q, g = queries[0], out_grad[0]
    odd = lax.axis_index("ctx") & 1 == 1
    kv = jnp.stack([stored_key_state[0], stored_value_state[0]]).transpose(0, 2, 1, 3)
    kv, odd = lax.optimization_barrier((kv, odd))

    part_far = send(kv, -1, ahead)
    part_near_odd = send(kv, -1, even_to_odd)
    own_far = send(kv, 0, ahead)
    part_near_even = send(part_far, 0, odd_to_even)

    lse = by_group(logsumexp[0] * LOG2E, groups)
    dots = by_group(row_dots[0], groups)
    q, g, dq, own_grad = own_call(q, g, lse, dots, kv)
    dq, grad = earlier_call(q, g, lse, dots, dq, [[part_far]], False)
    part_far_home = send(grad, 1, back_two)
    own_far, dq = lax.optimization_barrier((own_far, dq))
    dq, grad = earlier_call(q, g, lse, dots, dq, [[own_far]], False)
    own_far_home = send(grad, 0, back_two)
    own_near = send(jnp.where(odd, own_far, kv), 0, swap)
    dq, grad = earlier_call(q, g, lse, dots, dq, [[part_near_odd, part_near_even]], False)
    part_near_home = send(grad, 1, back_one)
    dq, grad = earlier_call(q, g, lse, dots, dq, [[own_near]], True)
    own_near_home = send(grad, 0, back_one)

    total = own_grad + part_far_home.astype(F32) + part_near_home.astype(F32)
    total = total + own_far_home.astype(F32) + own_near_home.astype(F32)
    total = total.transpose(0, 2, 1, 3)
    return dq[None], total[0][None], total[1][None]


def solution(mesh):
    rows, vecs = P("doc", "ctx", None, None), P("doc", None, "ctx")
    return jax.shard_map(
        step,
        mesh=mesh,
        in_specs=(rows, rows, rows, rows, vecs, vecs),
        out_specs=(rows, rows, rows),
        check_vma=False,
    )
```

```python
import functools
import math

import jax
import jax.numpy as jnp
from jax import lax
from jax.experimental import pallas as pl
from jax.experimental.pallas import tpu as pltpu
from jax.sharding import PartitionSpec as P


LOG2E = math.log2(math.e)
F32, BF16 = jnp.float32, jnp.bfloat16
NT = (((1,), (1,)), ((), ()))
NN = (((1,), (0,)), ((), ()))


def mm(a, b, dims):
    return lax.dot_general(a, b, dims, preferred_element_type=F32)


def columns(width, q, g, lse, dot, sl, k, v, mask):
    qc, gc = q[sl, :], g[sl, :]
    s = mm(k, qc, NT)
    p = jnp.exp2(s * (LOG2E * width**-0.5) - lse[:, sl])
    if mask is not None:
        p = jnp.where(mask, p, 0.0)
    dv = mm(p.astype(BF16), gc, NN)
    dp = mm(v, gc, NT)
    ds = (p * (dp - dot[:, sl])).astype(BF16)
    dk = mm(ds, qc, NN)
    dq = mm(k.T, ds, NN).T
    return dq, dk, dv


def own_group(cw, step, q, g, lse, dot, keys, values, save, out_k, out_v):
    n, width = q.shape
    heads = n // keys.shape[0]
    parts = []
    for c in range(n // cw):
        sl = pl.ds(c * cw, cw)
        seen = pl.cdiv((c + 1) * cw // heads, step) * step
        key = lax.broadcasted_iota(jnp.int32, (seen, cw), 0)
        column = lax.broadcasted_iota(jnp.int32, (seen, cw), 1) + c * cw
        mask = key * heads <= column
        dqc, dkc, dvc = columns(width, q, g, lse, dot, sl, keys[:seen, :], values[:seen, :], mask)
        save(sl, dqc)
        parts.append((dkc * width**-0.5, dvc))
    done = 0
    for seen in sorted({dk.shape[0] for dk, _ in parts}):
        rows = [(dk[done:seen], dv[done:seen]) for dk, dv in parts if dk.shape[0] >= seen]
        out_k[done:seen, :] = sum(dk for dk, _ in rows)
        out_v[done:seen, :] = sum(dv for _, dv in rows)
        done = seen


def own_first_kernel(cw, step, q_hbm, g_hbm, lse_ref, dot_ref, kv_ref, q_ref, g_ref, dq_ref, out_ref, sems):
    groups, tokens, heads, width = q_ref.shape
    n, half = tokens * heads, out_ref.shape[1]

    def copies(j):
        rows = pl.ds(pl.multiple_of(j * heads, heads), heads)
        return [
            pltpu.make_async_copy(src.at[:, rows, :], dst.at[j], sems.at[i, j])
            for i, (src, dst) in enumerate(((q_hbm, q_ref), (g_hbm, g_ref)))
        ]

    for j in range(groups):
        for copy in copies(j):
            copy.start()

    def group(j, carry):
        for copy in copies(j):
            copy.wait()
        dq_rows = dq_ref.at[j].reshape(n, width)

        def save(sl, dqc):
            dq_rows[sl, :] = dqc

        own_group(
            cw,
            step,
            q_ref.at[j].reshape(n, width),
            g_ref.at[j].reshape(n, width),
            lse_ref.at[j],
            dot_ref.at[j],
            kv_ref.at[0, j],
            kv_ref.at[1, j],
            save,
            out_ref.at[0, j],
            out_ref.at[1, j],
        )
        return carry

    lax.fori_loop(0, half, group, 0)
    for j in range(half, groups):
        dq_ref[j] = jnp.zeros(dq_ref.shape[1:], F32)
        for copy in copies(j):
            copy.wait()


def own_last_kernel(cw, step, q_ref, g_ref, lse_ref, dot_ref, kv_ref, prev_ref, _, dq_hbm, out_ref, dq_ref, sems):
    groups, tokens, heads, width = q_ref.shape
    n, half = tokens * heads, groups - out_ref.shape[1]

    def copy_out(j):
        rows = pl.ds(pl.multiple_of(j * heads, heads), heads)
        return pltpu.make_async_copy(dq_ref.at[j - half], dq_hbm.at[:, rows, :], sems.at[j - half])

    def group(j, carry):
        dq_rows, prev = dq_ref.at[j - half].reshape(n, width), prev_ref.at[j].reshape(n, width)

        def save(sl, dqc):
            dq_rows[sl, :] = (dqc + prev[sl, :]) * width**-0.5

        own_group(
            cw,
            step,
            q_ref.at[j].reshape(n, width),
            g_ref.at[j].reshape(n, width),
            lse_ref.at[j],
            dot_ref.at[j],
            kv_ref.at[0, j],
            kv_ref.at[1, j],
            save,
            out_ref.at[0, j - half],
            out_ref.at[1, j - half],
        )
        copy_out(j).start()
        return carry

    lax.fori_loop(half, groups, group, 0)
    for j in range(half, groups):
        copy_out(j).wait()


def earlier_kernel(cw, merge, ended, q_ref, g_ref, lse_ref, dot_ref, prev_ref, *rest):
    n_in = sum(merge)
    in_refs, dq_out, rest = rest[:n_in], rest[n_in], rest[n_in + 1 :]
    outs, ends = rest[: len(merge)], rest[len(merge) :]
    groups, tokens, heads, width = q_ref.shape
    n = tokens * heads

    def copy_out(j):
        rows = pl.ds(pl.multiple_of(j * heads, heads), heads)
        return pltpu.make_async_copy(ends[1].at[j], ends[0].at[:, rows, :], ends[2].at[j])

    def group(last, j, carry):
        q, g = q_ref.at[j].reshape(n, width), g_ref.at[j].reshape(n, width)
        prev = prev_ref.at[j].reshape(n, width)
        dq_rows = (ends[1] if last else dq_out).at[j].reshape(n, width)
        blocks, refs = [], in_refs
        for count in merge:
            k, v = refs[0][0, j], refs[0][1, j]
            for other in refs[1:count]:
                k, v = k + other[0, j], v + other[1, j]
            blocks.append((k, v))
            refs = refs[count:]
        k = jnp.concatenate([k for k, _ in blocks], axis=0)
        v = jnp.concatenate([v for _, v in blocks], axis=0)
        dk = dv = None
        for c in range(n // cw):
            sl = pl.ds(c * cw, cw)
            dqc, dkc, dvc = columns(width, q, g, lse_ref.at[j], dot_ref.at[j], sl, k, v, None)
            dqc = dqc + prev[sl, :]
            dq_rows[sl, :] = dqc * width**-0.5 if last else dqc
            dk = dkc if dk is None else dk + dkc
            dv = dvc if dv is None else dv + dvc
        if last:
            copy_out(j).start()
        dk = dk * width**-0.5
        for i, out in enumerate(outs):
            out[0, j] = dk[i * tokens : (i + 1) * tokens].astype(BF16)
            out[1, j] = dv[i * tokens : (i + 1) * tokens].astype(BF16)
        return carry

    if ended:
        lax.fori_loop(0, ended, functools.partial(group, True), 0)
    lax.fori_loop(ended, groups, functools.partial(group, False), 0)
    for j in range(ended):
        copy_out(j).wait()


VMEM = pl.BlockSpec(memory_space=pltpu.VMEM)
HBM = pl.BlockSpec(memory_space=pltpu.HBM)


def in_hbm(x):
    return pltpu.with_memory_space_constraint(x, pltpu.HBM)


def in_vmem(x):
    return pltpu.with_memory_space_constraint(x, pltpu.VMEM)


def work(blocks, rows, tokens, width):
    pairs = blocks * rows * tokens
    return pl.CostEstimate(flops=10 * pairs * width, transcendentals=pairs, bytes_accessed=16 << 20)


def own_first_call(q, g, lse, dots, kv, half):
    tokens, heads, width = q.shape
    groups = kv.shape[1]
    shape = (groups, tokens, heads // groups, width)
    return pl.pallas_call(
        functools.partial(own_first_kernel, 1024, 128),
        in_specs=[HBM, HBM, VMEM, VMEM, VMEM],
        out_specs=[VMEM, VMEM, VMEM, VMEM],
        out_shape=[
            pltpu.VMEM(shape, BF16),
            pltpu.VMEM(shape, BF16),
            pltpu.VMEM(shape, F32),
            jax.ShapeDtypeStruct((2, half, tokens, width), F32),
        ],
        scratch_shapes=[pltpu.SemaphoreType.DMA((2, groups))],
        compiler_params=pltpu.CompilerParams(vmem_limit_bytes=LIMIT),
        cost_estimate=work(1, heads * tokens, tokens, width),
        name="own_first",
    )(in_hbm(q), in_hbm(g), lse, dots, kv)


def own_last_call(q, g, lse, dots, kv, prev, dq, half):
    groups, tokens, per, width = q.shape
    rest = groups - half
    return pl.pallas_call(
        functools.partial(own_last_kernel, 1024, 128),
        in_specs=[VMEM, VMEM, VMEM, VMEM, VMEM, VMEM, HBM],
        out_specs=[HBM, VMEM],
        out_shape=[
            jax.ShapeDtypeStruct(dq.shape, F32),
            jax.ShapeDtypeStruct((2, rest, tokens, width), F32),
        ],
        scratch_shapes=[
            pltpu.VMEM((rest, tokens, per, width), F32),
            pltpu.SemaphoreType.DMA((rest,)),
        ],
        input_output_aliases={6: 0},
        compiler_params=pltpu.CompilerParams(vmem_limit_bytes=LIMIT),
        cost_estimate=work(1, groups * per * tokens, tokens, width),
        name="own_last",
    )(in_vmem(q), in_vmem(g), lse, dots, kv, in_vmem(prev), in_hbm(dq))


def earlier_call(q, g, lse, dots, prev, blocks, ended=0):
    groups, tokens, per, width = q.shape
    parts = [part for block in blocks for part in block]
    merge = tuple(len(block) for block in blocks)
    out_specs = [VMEM] * (1 + len(blocks))
    out_shape = [pltpu.VMEM(q.shape, F32)]
    out_shape += [jax.ShapeDtypeStruct(parts[0].shape, BF16)] * len(blocks)
    scratch = []
    if ended:
        out_specs.append(HBM)
        out_shape.append(jax.ShapeDtypeStruct((tokens, groups * per, width), F32))
        held = (ended, tokens, per, width)
        scratch = [pltpu.VMEM(held, F32), pltpu.SemaphoreType.DMA((ended,))]
    return pl.pallas_call(
        functools.partial(earlier_kernel, 512 if len(blocks) > 1 else 1024, merge, ended),
        in_specs=[VMEM] * (5 + len(parts)),
        out_specs=out_specs,
        out_shape=out_shape,
        scratch_shapes=scratch,
        input_output_aliases={4: 0},
        compiler_params=pltpu.CompilerParams(vmem_limit_bytes=LIMIT),
        cost_estimate=work(len(blocks), groups * per * tokens, tokens, width),
    )(in_vmem(q), in_vmem(g), lse, dots, in_vmem(prev), *parts)


LIMIT = 24 << 20


def send(x, by_doc, to):
    docs, ctxs = lax.axis_size("doc"), lax.axis_size("ctx")
    pairs = []
    for d in range(docs):
        for c in range(ctxs):
            t = to(c)
            if t is not None and 0 <= t < ctxs:
                pairs.append((d * ctxs + c, (d + by_doc) % docs * ctxs + t))
    return lax.ppermute(x, ("doc", "ctx"), pairs)


def ahead(c):
    return c + 2


def back_one(c):
    return c - 1


def back_two(c):
    return c - 2


def swap(c):
    return c ^ 1


def even_to_odd(c):
    return c + 1 if c % 2 == 0 else None


def odd_to_even(c):
    return c - 1 if c % 2 == 1 else None


def by_group(x, groups):
    heads, tokens = x.shape
    return x.reshape(groups, heads // groups, tokens).transpose(0, 2, 1).reshape(groups, 1, -1)


def step(queries, stored_key_state, stored_value_state, out_grad, logsumexp, row_dots):
    groups = stored_key_state.shape[2]
    q, g = queries[0], out_grad[0]
    odd = lax.axis_index("ctx") & 1 == 1
    kv = jnp.stack([stored_key_state[0], stored_value_state[0]]).transpose(0, 2, 1, 3)
    kv, odd = lax.optimization_barrier((kv, odd))

    part_far = send(kv, -1, ahead)
    part_near_odd = send(kv, -1, even_to_odd)
    own_far = send(kv, 0, ahead)
    part_near_even = send(part_far, 0, odd_to_even)

    lse = by_group(logsumexp[0] * LOG2E, groups)
    dots = by_group(row_dots[0], groups)
    half = groups // 2
    q, g, dq, own_grad = own_first_call(q, g, lse, dots, kv, half)
    dq, grad = earlier_call(q, g, lse, dots, dq, [[part_far]])
    part_far_home = send(grad, 1, back_two)
    own_far, dq = lax.optimization_barrier((own_far, dq))
    dq, grad = earlier_call(q, g, lse, dots, dq, [[own_far]])
    own_far_home = send(grad, 0, back_two)
    own_near = send(jnp.where(odd, own_far, kv), 0, swap)
    dq, grad = earlier_call(q, g, lse, dots, dq, [[part_near_odd, part_near_even]])
    part_near_home = send(grad, 1, back_one)
    dq, grad, query_grad = earlier_call(q, g, lse, dots, dq, [[own_near]], half)
    own_near_home = send(grad, 0, back_one)
    query_grad, own_rest = own_last_call(q, g, lse, dots, kv, dq, query_grad, half)

    total = jnp.concatenate([own_grad, own_rest], axis=1)
    total = total + part_far_home.astype(F32) + part_near_home.astype(F32)
    total = total + own_far_home.astype(F32) + own_near_home.astype(F32)
    total = total.transpose(0, 2, 1, 3)
    return query_grad[None], total[0][None], total[1][None]


def solution(mesh):
    rows, vecs = P("doc", "ctx", None, None), P("doc", None, "ctx")
    return jax.shard_map(
        step,
        mesh=mesh,
        in_specs=(rows, rows, rows, rows, vecs, vecs),
        out_specs=(rows, rows, rows),
        check_vma=False,
    )
```
